128 devices in a mesh: data: 1, seq: 128 (over z, y, x, core).
Axes of the slice: x: 4, y: 4, z: 4, core: 2. Of those that a mesh axis runs over, the one named last changes fastest.
Arguments:
- tokens: bfloat16 [32, 16384, 384], P('data', 'seq')
- lengths: int32 [32], P('data')
- slot_params: bfloat16 [384, 128], replicated
- logit_scale: float32 [1], replicated
- w_in: bfloat16 [128, 384, 1536], P('seq')
- w_out: bfloat16 [128, 1536, 384], P('seq')
Outputs:
- output: bfloat16 [32, 16384, 384], P('data', 'seq')
All inputs are finite; a program needn't handle non-finite values.
Results may differ from the reference program's by a relative error of at most 0.0157012.
Values are sent between devices in bfloat16 or wider.
A program may use at most 1 GiB of HBM per device.

```python
import jax
import jax.numpy as jnp
from jax import lax

BATCH = 32
TOKENS = 16384
D_MODEL = 384
FF_DIM = 1536
EXPERTS = 128
SLOTS = 1
NUM_SLOTS = EXPERTS * SLOTS


def setup_inputs(seed: int = 0, part: int = 0) -> dict:
    base_key = jax.random.key(seed)
    k_phi, k_win, k_wout, k_gain = jax.random.split(base_key, 4)
    part_key = jax.random.fold_in(base_key, part)
    k_sel, k_noise, k_len = jax.random.split(part_key, 3)
    slot_params = jax.random.normal(k_phi, (D_MODEL, NUM_SLOTS), jnp.float32)
    chosen = jax.random.randint(k_sel, (BATCH, TOKENS), 0, NUM_SLOTS)
    noise = jax.random.normal(k_noise, (BATCH, TOKENS, D_MODEL), jnp.float32)
    tokens = jnp.take(slot_params.T, chosen, axis=0) + noise
    lengths = jax.random.randint(k_len, (BATCH,), 1, TOKENS + 1)
    logit_scale = jax.random.uniform(k_gain, (1,), jnp.float32, 6.0, 9.0)
    w_in = jax.random.normal(k_win, (EXPERTS, D_MODEL, FF_DIM), jnp.float32) * D_MODEL ** -0.5
    w_out = jax.random.normal(k_wout, (EXPERTS, FF_DIM, D_MODEL), jnp.float32) * FF_DIM ** -0.5
    return {
        "tokens": tokens.astype(jnp.bfloat16),
        "lengths": lengths.astype(jnp.int32),
        "slot_params": slot_params.astype(jnp.bfloat16),
        "logit_scale": logit_scale,
        "w_in": w_in.astype(jnp.bfloat16),
        "w_out": w_out.astype(jnp.bfloat16),
    }


def reference(tokens, lengths, slot_params, logit_scale, w_in, w_out):
    params_f32 = slot_params.astype(jnp.float32)
    col_inv = lax.rsqrt(jnp.sum(params_f32 * params_f32, axis=0, keepdims=True) + 1e-6)
    phi_norm = (params_f32 * (logit_scale[0] * col_inv)).astype(jnp.bfloat16)
    positions = jnp.arange(TOKENS)

    def row_logits(row_tokens):
        tok_f32 = row_tokens.astype(jnp.float32)
        tok_norm = (tok_f32 * lax.rsqrt(jnp.sum(tok_f32 * tok_f32, axis=-1, keepdims=True) + 1e-6)).astype(jnp.bfloat16)
        return jnp.dot(tok_norm, phi_norm, preferred_element_type=jnp.float32)

    def dispatch_row(row_args):
        row_tokens, row_len = row_args
        logits = row_logits(row_tokens)
        is_valid = (positions < row_len)[:, None]
        col_max = jnp.max(jnp.where(is_valid, logits, -jnp.inf), axis=0)
        disp_w = jnp.where(is_valid, jnp.exp(logits - col_max[None, :]), 0.0)
        col_sum = jnp.sum(disp_w, axis=0)
        slot_sum = jnp.dot(disp_w.astype(jnp.bfloat16).T, row_tokens, preferred_element_type=jnp.float32)
        return (slot_sum / col_sum[:, None]).astype(jnp.bfloat16)

    slot_in = lax.map(dispatch_row, (tokens, lengths))
    by_expert = slot_in.reshape(BATCH, EXPERTS, SLOTS, D_MODEL).transpose(1, 0, 2, 3).reshape(EXPERTS, BATCH * SLOTS, D_MODEL)

    def expert_ffn(exp_args):
        exp_in, exp_w_in, exp_w_out = exp_args
        hidden = jax.nn.gelu(jnp.dot(exp_in, exp_w_in, preferred_element_type=jnp.float32)).astype(jnp.bfloat16)
        return jnp.dot(hidden, exp_w_out, preferred_element_type=jnp.float32).astype(jnp.bfloat16)

    expert_out = lax.map(expert_ffn, (by_expert, w_in, w_out))
    slot_out = expert_out.reshape(EXPERTS, BATCH, SLOTS, D_MODEL).transpose(1, 0, 2, 3).reshape(BATCH, NUM_SLOTS, D_MODEL)

    def combine_row(row_args):
        row_tokens, row_len, row_slots = row_args
        logits = row_logits(row_tokens)
        is_valid = (positions < row_len)[:, None]
        combine_w = jax.nn.softmax(logits, axis=-1).astype(jnp.bfloat16)
        mixed = jnp.dot(combine_w, row_slots, preferred_element_type=jnp.float32).astype(jnp.bfloat16)
        return jnp.where(is_valid, mixed, jnp.zeros_like(mixed))

    return lax.map(combine_row, (tokens, lengths, slot_out))
```

```python
import functools

import jax
import jax.numpy as jnp
from jax import lax
from jax.experimental import pallas as pl
from jax.experimental.pallas import tpu as pltpu
from jax.sharding import PartitionSpec as P

F32, BF16 = jnp.float32, jnp.bfloat16
COLOR_ROWS = (11, 11, 10)
COLOR_START = (0, 11, 22)
COLOR_HALF = (6, 6, 5)
STRIDE = {"z": 32, "y": 8, "x": 2}
COLOR_AXES = (("z", "y", "x"), ("y", "x", "z"), ("x", "z", "y"))
COPIES = 160


def slots_kernel(
    len_ref, scale_ref, tok_hbm, phi_ref, win_hbm, wout_hbm,
    comb_hbm, gat_hbm,
    tok, win, wout, comb, part, swap, chip, relay, line,
    two_out, two_in, three_out, three_in, z_own, z_out, z_swap, z_in, lanes, gat,
    send_sem, recv_sem, local_sem,
):
    num_rows, tok_count, width = tok.shape
    me = lax.axis_index("seq")
    core = lax.rem(me, 2)
    at = {axis: lax.rem(lax.div(me, stride), 4) for axis, stride in STRIDE.items()}
    partner = me + 1 - 2 * core

    def peer(axis, step):
        return me + (lax.rem(at[axis] + step, 4) - at[axis]) * STRIDE[axis]

    copies = []

    def push(src, dst, device):
        index = len(copies)
        copy = pltpu.make_async_remote_copy(
            src_ref=src, dst_ref=dst, send_sem=send_sem.at[index], recv_sem=recv_sem.at[index],
            device_id={"seq": device}, device_id_type=pl.DeviceIdType.MESH,
        )
        copy.start()
        copies.append(copy)
        return copy

    chunks = []
    for half in range(2):
        for color in range(3):
            start, rows, cut = COLOR_START[color], COLOR_ROWS[color], COLOR_HALF[color]
            chunks.append((color, half, start + half * cut, cut if half == 0 else rows - cut))

    barrier = pltpu.get_barrier_semaphore()
    neighbours = [partner] + [peer(axis, step) for axis in STRIDE for step in (1, 2, 3)]
    for other in neighbours:
        pl.semaphore_signal(barrier, inc=1, device_id={"seq": other}, device_id_type=pl.DeviceIdType.MESH)

    loads = []
    for index, (_, _, lo, count) in enumerate(chunks):
        load = pltpu.make_async_copy(tok_hbm.at[pl.ds(lo, count)], tok.at[pl.ds(lo, count)], local_sem.at[index])
        load.start()
        loads.append(load)
    load_in = pltpu.make_async_copy(win_hbm.at[0], win, local_sem.at[6])
    load_out = pltpu.make_async_copy(wout_hbm.at[0], wout, local_sem.at[7])
    load_in.start()
    load_out.start()

    params = phi_ref[...].astype(F32)
    col_inv = lax.rsqrt(jnp.sum(params * params, axis=0, keepdims=True) + 1e-6)
    phi = (params * (scale_ref[0] * col_inv)).astype(BF16)
    slot = lax.broadcasted_iota(jnp.int32, (128, 128), 0)
    place = lax.broadcasted_iota(jnp.int32, (128, 128), 1)
    phis = []
    for color in range(3):
        owner = (core + (place >> 6)) & 1
        for depth, axis in enumerate(COLOR_AXES[color]):
            owner = owner + STRIDE[axis] * ((at[axis] + (place >> (4 - 2 * depth))) & 3)
        pick = jnp.where(slot == owner, 1.0, 0.0).astype(BF16)
        phis.append(jnp.dot(phi, pick, preferred_element_type=F32).astype(BF16))
    z_own[...] = jnp.ones_like(z_own)
    position = me * tok_count + lax.broadcasted_iota(jnp.int32, (tok_count, 128), 0)

    def dispatch(chunk):
        color, _, lo, count = chunk

        def body(step, carry):
            row = lo + step
            x = tok[row]
            xf = x.astype(F32)
            inv = lax.rsqrt(jnp.sum(xf * xf, axis=-1, keepdims=True) + 1e-6)
            logits = jnp.dot((xf * inv).astype(BF16), phis[color], preferred_element_type=F32)
            weight = jnp.exp(logits)
            comb[row] = (weight / jnp.sum(weight, axis=-1, keepdims=True)).astype(BF16)
            weight = jnp.where(position < len_ref[row], weight, 0.0)
            z_own[color, pl.ds(row - COLOR_START[color], 1), :] = jnp.sum(weight, axis=0, keepdims=True)
            total = lax.dot_general(
                weight.astype(BF16), x, (((0,), (0,)), ((), ())), preferred_element_type=F32
            ).astype(BF16)
            part[row, 0] = total[:64]
            part[row, 1] = total[64:]
            return carry

        lax.fori_loop(0, count, body, 0)

    def start_swap(chunk):
        color, half, lo, count = chunk
        rows = pl.ds(lo, count)
        out = [push(part.at[rows, 1], swap.at[rows], partner)]
        if half == 1:
            z_out[0, color] = pltpu.roll(z_own[color], 64, 1)
            out.append(push(z_out.at[0, color], z_swap.at[color], partner))
        return out

    def line_z(color, phase, total):
        z_out[phase, color] = total
        axis = COLOR_AXES[color][phase - 1]
        return [push(z_out.at[phase, color], z_in.at[phase - 1, color, step - 1], peer(axis, step)) for step in (1, 2, 3)]

    def sum_z(color, phase, arrivals):
        total = z_out[phase, color]
        for step in (1, 2, 3):
            arrivals[step - 1].wait_recv()
            shift = 128 - step * (64 >> (2 * phase))
            total = total + pltpu.roll(z_in[phase - 1, color, step - 1], shift, 1)
        return total

    relays, cleans, z_one = {}, {}, {}

    def start_line(chunk, arrivals):
        color, half, lo, count = chunk
        for copy in arrivals:
            copy.wait_recv()

        def body(step, carry):
            row = lo + step
            both = part[row, 0].astype(F32) + swap[row].astype(F32)
            chip[row] = both.astype(BF16).reshape(4, 16, width)
            return carry

        lax.fori_loop(0, count, body, 0)
        rows = pl.ds(lo, count)
        axis = COLOR_AXES[color][0]
        away, back = (1, 3) if half == 0 else (3, 1)
        relays[color, half] = push(chip.at[rows, 2], relay.at[rows], peer(axis, away))
        cleans[color, half] = push(chip.at[rows, back], line.at[half, rows], peer(axis, back))
        if half == 1:
            z_one[color] = line_z(color, 1, z_own[color] + z_swap[color])

    for chunk, load in zip(chunks[:1], loads[:1]):
        load.wait()
        dispatch(chunk)
    pl.semaphore_wait(barrier, len(neighbours))
    pending = start_swap(chunks[0])
    for index in range(len(chunks)):
        following = None
        if index + 1 < len(chunks):
            loads[index + 1].wait()
            dispatch(chunks[index + 1])
            following = start_swap(chunks[index + 1])
        start_line(chunks[index], pending)
        pending = following
    store_comb = pltpu.make_async_copy(comb, comb_hbm, local_sem.at[8])
    store_comb.start()

    seconds = {}
    for chunk in chunks:
        color, half, lo, count = chunk
        axis = COLOR_AXES[color][0]
        relays[color, half].wait_recv()
        away = 1 if half == 0 else 3

        def body(step, carry):
            row = lo + step
            chip[row, away] = (chip[row, away].astype(F32) + relay[row].astype(F32)).astype(BF16)
            return carry

        lax.fori_loop(0, count, body, 0)
        rows = pl.ds(lo, count)
        seconds[color, half] = push(chip.at[rows, away], line.at[1 - half, rows], peer(axis, away))

    left = lax.broadcasted_iota(jnp.int32, (256, 256), 0)
    right = lax.broadcasted_iota(jnp.int32, (256, 256), 1)
    turn = jnp.where(((left >> 4) == (right & 15)) & ((left & 15) == (right >> 4)), 1.0, 0.0).astype(BF16)

    twos, z_two = {}, {}
    for color in range(3):
        rows, start = COLOR_ROWS[color], COLOR_START[color]
        span = pl.ds(start, rows)
        for half in range(2):
            cleans[color, half].wait_recv()
            seconds[color, half].wait_recv()
        z_two[color] = line_z(color, 2, sum_z(color, 1, z_one[color]))
        total = chip[span, 0].astype(F32) + line[0, span].astype(F32) + line[1, span].astype(F32)
        total = total.astype(BF16).reshape(rows * 16, width)
        turned = jnp.dot(turn[:, : rows * 16], total, preferred_element_type=F32)
        two_out[color] = turned.astype(BF16).reshape(4, 4, 16, width)
        axis = COLOR_AXES[color][1]
        twos[color] = [push(two_out.at[color, step], two_in.at[color, step - 1], peer(axis, step)) for step in (1, 2, 3)]

    threes, z_three = {}, {}
    for color in range(3):
        z_three[color] = line_z(color, 3, sum_z(color, 2, z_two[color]))
        total = two_out[color, 0].astype(F32)
        for step in (1, 2, 3):
            twos[color][step - 1].wait_recv()
            total = total + two_in[color, step - 1].astype(F32)
        three_out[color] = total.astype(BF16)
        axis = COLOR_AXES[color][2]
        threes[color] = [push(three_out.at[color, step], three_in.at[color, step - 1], peer(axis, step)) for step in (1, 2, 3)]

    slot_in = []
    for color in range(3):
        z_sum = sum_z(color, 3, z_three[color])
        total = three_out[color, 0].astype(F32)
        for step in (1, 2, 3):
            threes[color][step - 1].wait_recv()
            total = total + three_in[color, step - 1].astype(F32)
        slot_in.append((total / z_sum[:, :1]).astype(BF16))
    slot_in = jnp.concatenate(slot_in, axis=0)

    load_in.wait()
    load_out.wait()
    slot_out = jnp.zeros((48, width), F32)
    for piece in range(3):
        cols = pl.ds(piece * 512, 512)
        hidden = jnp.dot(slot_in, win[:, cols], preferred_element_type=F32)
        hidden = jax.nn.gelu(hidden).astype(BF16)
        slot_out = slot_out + jnp.dot(hidden, wout[cols, :], preferred_element_type=F32)
    slot_out = slot_out.astype(BF16)

    firsts = {}
    for color in range(3):
        lanes[color, 0, 0] = slot_out[16 * color : 16 * color + 16]
        axis = COLOR_AXES[color][2]
        firsts[color] = [push(lanes.at[color, 0, 0], lanes.at[color, 0, 4 - step], peer(axis, step)) for step in (1, 2, 3)]
    nexts = {}
    for color in range(3):
        for copy in firsts[color]:
            copy.wait_recv()
        axis = COLOR_AXES[color][1]
        nexts[color] = [push(lanes.at[color, 0], lanes.at[color, 4 - step], peer(axis, step)) for step in (1, 2, 3)]

    outs, across = {}, {color: [] for color in range(3)}

    def halves(color):
        start, rows, cut = COLOR_START[color], COLOR_ROWS[color], COLOR_HALF[color]
        return pl.ds(start, cut), pl.ds(start + cut, rows - cut)

    for color in range(3):
        rows, start = COLOR_ROWS[color], COLOR_START[color]
        for copy in nexts[color]:
            copy.wait_recv()
        turned = jnp.dot(turn[: rows * 16], lanes[color].reshape(256, width), preferred_element_type=F32)
        gat[pl.ds(start, rows), 0, 0] = turned.astype(BF16).reshape(rows, 16, width)
        early, late = halves(color)
        axis = COLOR_AXES[color][0]
        up, down = peer(axis, 1), peer(axis, 3)
        outs[color] = [
            push(gat.at[early, 0, 0], gat.at[early, 0, 3], up),
            push(gat.at[late, 0, 0], gat.at[late, 0, 1], down),
            push(gat.at[late, 0, 0], gat.at[late, 0, 3], up),
            push(gat.at[early, 0, 0], gat.at[early, 0, 1], down),
        ]
        span = pl.ds(start, rows)
        across[color].append(push(gat.at[span, 0, 0], gat.at[span, 1, 0], partner))

    hops = {}
    for color in range(3):
        early, late = halves(color)
        axis = COLOR_AXES[color][0]
        up, down = peer(axis, 1), peer(axis, 3)
        outs[color][0].wait_recv()
        first = push(gat.at[early, 0, 3], gat.at[early, 0, 2], up)
        outs[color][1].wait_recv()
        second = push(gat.at[late, 0, 1], gat.at[late, 0, 2], down)
        hops[color] = [first, second]
        across[color].append(push(gat.at[early, 0, 3], gat.at[early, 1, 3], partner))
        across[color].append(push(gat.at[late, 0, 1], gat.at[late, 1, 1], partner))
    for color in range(3):
        early, late = halves(color)
        outs[color][2].wait_recv()
        across[color].append(push(gat.at[late, 0, 3], gat.at[late, 1, 3], partner))
        outs[color][3].wait_recv()
        across[color].append(push(gat.at[early, 0, 1], gat.at[early, 1, 1], partner))
    for color in range(3):
        early, late = halves(color)
        hops[color][0].wait_recv()
        across[color].append(push(gat.at[early, 0, 2], gat.at[early, 1, 2], partner))
        hops[color][1].wait_recv()
        across[color].append(push(gat.at[late, 0, 2], gat.at[late, 1, 2], partner))
    stores = [store_comb]
    for color in range(3):
        for copy in across[color]:
            copy.wait_recv()
        span = pl.ds(COLOR_START[color], COLOR_ROWS[color])
        store = pltpu.make_async_copy(gat.at[span], gat_hbm.at[span], local_sem.at[9 + color])
        store.start()
        stores.append(store)
    for copy in copies:
        copy.wait_send()
    for store in stores:
        store.wait()


def combine_kernel(len_ref, comb_ref, gat_ref, y_ref):
    count, tok_count, _ = comb_ref.shape
    base = pl.program_id(0) * count
    position = lax.axis_index("seq") * tok_count + lax.broadcasted_iota(jnp.int32, (tok_count, 1), 0)
    for step in range(count):
        mixed = jnp.dot(comb_ref[step], gat_ref[step], preferred_element_type=F32).astype(BF16)
        y_ref[step] = jnp.where(position < len_ref[base + step], mixed, jnp.zeros_like(mixed))


def solution(mesh):
    def shard_body(tok_blk, len_blk, slot_params, logit_scale, w_in_blk, w_out_blk):
        rows, toks, width = tok_blk.shape
        ff = w_in_blk.shape[2]
        slots = slot_params.shape[1]
        smem = pl.BlockSpec(memory_space=pltpu.SMEM)
        vmem = pl.BlockSpec(memory_space=pltpu.VMEM)
        hbm = pl.BlockSpec(memory_space=pl.ANY)
        comb, gat = pl.pallas_call(
            slots_kernel,
            name="slots",
            out_shape=(
                jax.ShapeDtypeStruct((rows, toks, slots), BF16),
                jax.ShapeDtypeStruct((rows, 2, 4, 16, width), BF16),
            ),
            in_specs=[smem, smem, hbm, vmem, hbm, hbm],
            out_specs=(hbm, hbm),
            scratch_shapes=[
                pltpu.VMEM((rows, toks, width), BF16),
                pltpu.VMEM((width, ff), BF16),
                pltpu.VMEM((ff, width), BF16),
                pltpu.VMEM((rows, toks, slots), BF16),
                pltpu.VMEM((rows, 2, 64, width), BF16),
                pltpu.VMEM((rows, 64, width), BF16),
                pltpu.VMEM((rows, 4, 16, width), BF16),
                pltpu.VMEM((rows, 16, width), BF16),
                pltpu.VMEM((2, rows, 16, width), BF16),
                pltpu.VMEM((3, 4, 4, 16, width), BF16),
                pltpu.VMEM((3, 3, 4, 16, width), BF16),
                pltpu.VMEM((3, 4, 16, width), BF16),
                pltpu.VMEM((3, 3, 16, width), BF16),
                pltpu.VMEM((3, 16, slots), F32),
                pltpu.VMEM((4, 3, 16, slots), F32),
                pltpu.VMEM((3, 16, slots), F32),
                pltpu.VMEM((3, 3, 3, 16, slots), F32),
                pltpu.VMEM((3, 4, 4, 16, width), BF16),
                pltpu.VMEM((rows, 2, 4, 16, width), BF16),
                pltpu.SemaphoreType.DMA((COPIES,)),
                pltpu.SemaphoreType.DMA((COPIES,)),
                pltpu.SemaphoreType.DMA((12,)),
            ],
            compiler_params=pltpu.CompilerParams(collective_id=0, has_side_effects=True, vmem_limit_bytes=60 * 1024 * 1024),
        )(len_blk, logit_scale, tok_blk, slot_params, w_in_blk, w_out_blk)
        gat = gat.reshape(rows, slots, width)
        block = 4
        return pl.pallas_call(
            combine_kernel,
            name="combine",
            out_shape=jax.ShapeDtypeStruct((rows, toks, width), BF16),
            grid=(rows // block,),
            in_specs=[
                smem,
                pl.BlockSpec((block, toks, slots), lambda i: (i, 0, 0)),
                pl.BlockSpec((block, slots, width), lambda i: (i, 0, 0)),
            ],
            out_specs=pl.BlockSpec((block, toks, width), lambda i: (i, 0, 0)),
        )(len_blk, comb, gat)

    return jax.shard_map(
        shard_body,
        mesh=mesh,
        in_specs=(P("data", "seq", None), P("data"), P(None, None), P(None), P("seq", None, None), P("seq", None, None)),
        out_specs=P("data", "seq", None),
        check_vma=False,
    )
```

```python
import functools

import jax
import jax.numpy as jnp
from jax import lax
from jax.experimental import pallas as pl
from jax.experimental.pallas import tpu as pltpu
from jax.sharding import PartitionSpec as P

F32, BF16 = jnp.float32, jnp.bfloat16
COLOR_ROWS = (11, 11, 10)
COLOR_START = (0, 11, 22)
COLOR_HALF = (6, 6, 5)
STRIDE = {"z": 32, "y": 8, "x": 2}
COLOR_AXES = (("z", "y", "x"), ("y", "x", "z"), ("x", "z", "y"))
COPIES = 160


def slots_kernel(
    len_ref, scale_ref, tok_hbm, phi_ref, win_hbm, wout_hbm,
    comb_hbm, gat_hbm,
    tok, win, wout, comb, part, swap, chip, relay, line,
    two_out, two_in, three_out, three_in, z_own, z_out, z_swap, z_in, lanes, gat,
    send_sem, recv_sem, local_sem,
):
    num_rows, tok_count, width = tok.shape
    me = lax.axis_index("seq")
    core = lax.rem(me, 2)
    at = {axis: lax.rem(lax.div(me, stride), 4) for axis, stride in STRIDE.items()}
    partner = me + 1 - 2 * core

    def peer(axis, step):
        return me + (lax.rem(at[axis] + step, 4) - at[axis]) * STRIDE[axis]

    copies = []

    def push(src, dst, device):
        index = len(copies)
        copy = pltpu.make_async_remote_copy(
            src_ref=src, dst_ref=dst, send_sem=send_sem.at[index], recv_sem=recv_sem.at[index],
            device_id={"seq": device}, device_id_type=pl.DeviceIdType.MESH,
        )
        copy.start()
        copies.append(copy)
        return copy

    chunks = []
    for half in range(2):
        for color in range(3):
            start, rows, cut = COLOR_START[color], COLOR_ROWS[color], COLOR_HALF[color]
            chunks.append((color, half, start + half * cut, cut if half == 0 else rows - cut))

    barrier = pltpu.get_barrier_semaphore()
    neighbours = [partner] + [peer(axis, step) for axis in STRIDE for step in (1, 2, 3)]
    for other in neighbours:
        pl.semaphore_signal(barrier, inc=1, device_id={"seq": other}, device_id_type=pl.DeviceIdType.MESH)

    loads = []
    for index, (_, _, lo, count) in enumerate(chunks):
        load = pltpu.make_async_copy(tok_hbm.at[pl.ds(lo, count)], tok.at[pl.ds(lo, count)], local_sem.at[index])
        load.start()
        loads.append(load)
    load_in = pltpu.make_async_copy(win_hbm.at[0], win, local_sem.at[6])
    load_out = pltpu.make_async_copy(wout_hbm.at[0], wout, local_sem.at[7])
    load_in.start()
    load_out.start()

    with jax.named_scope("setup"):
        params = phi_ref[...].astype(F32)
        col_inv = lax.rsqrt(jnp.sum(params * params, axis=0, keepdims=True) + 1e-6)
        phi = (params * (scale_ref[0] * col_inv)).astype(BF16)
        slot = lax.broadcasted_iota(jnp.int32, (128, 128), 0)
        place = lax.broadcasted_iota(jnp.int32, (128, 128), 1)
        phis = []
        for color in range(3):
            owner = (core + (place >> 6)) & 1
            for depth, axis in enumerate(COLOR_AXES[color]):
                owner = owner + STRIDE[axis] * ((at[axis] + (place >> (4 - 2 * depth))) & 3)
            pick = jnp.where(slot == owner, 1.0, 0.0).astype(BF16)
            phis.append(jnp.dot(phi, pick, preferred_element_type=F32).astype(BF16))
        z_own[...] = jnp.ones_like(z_own)
        position = me * tok_count + lax.broadcasted_iota(jnp.int32, (tok_count, 128), 0)
    def dispatch(chunk):
        color, _, lo, count = chunk
        xs = [tok[lo + step] for step in range(count)]
        squares = [jnp.sum(x.astype(F32) * x.astype(F32), axis=-1, keepdims=True) for x in xs]
        norms = [(x.astype(F32) * lax.rsqrt(square + 1e-6)).astype(BF16) for x, square in zip(xs, squares)]
        weights = [jnp.exp(jnp.dot(norm, phis[color], preferred_element_type=F32)) for norm in norms]
        masked = [jnp.where(position < len_ref[lo + step], weight, 0.0) for step, weight in enumerate(weights)]
        totals = [
            lax.dot_general(weight.astype(BF16), x, (((0,), (0,)), ((), ())), preferred_element_type=F32).astype(BF16)
            for weight, x in zip(masked, xs)
        ]
        for step in range(count):
            row = lo + step
            part[row, 0] = totals[step][:64]
            part[row, 1] = totals[step][64:]
            at_row = row - COLOR_START[color]
            z_own[color, at_row : at_row + 1, :] = jnp.sum(masked[step], axis=0, keepdims=True)
            comb[row] = (weights[step] / jnp.sum(weights[step], axis=-1, keepdims=True)).astype(BF16)

    def start_swap(chunk):
        color, half, lo, count = chunk
        rows = pl.ds(lo, count)
        out = [push(part.at[rows, 1], swap.at[rows], partner)]
        if half == 1:
            z_out[0, color] = pltpu.roll(z_own[color], 64, 1)
            out.append(push(z_out.at[0, color], z_swap.at[color], partner))
        return out

    def line_z(color, phase, total):
        z_out[phase, color] = total
        axis = COLOR_AXES[color][phase - 1]
        return [push(z_out.at[phase, color], z_in.at[phase - 1, color, step - 1], peer(axis, step)) for step in (1, 2, 3)]

    def sum_z(color, phase, arrivals):
        total = z_out[phase, color]
        for step in (1, 2, 3):
            arrivals[step - 1].wait_recv()
            shift = 128 - step * (64 >> (2 * phase))
            total = total + pltpu.roll(z_in[phase - 1, color, step - 1], shift, 1)
        return total

    relays, cleans, z_one = {}, {}, {}

    def start_line(chunk, arrivals):
        color, half, lo, count = chunk
        for copy in arrivals:
            copy.wait_recv()

        def body(step, carry):
            row = lo + step
            both = part[row, 0].astype(F32) + swap[row].astype(F32)
            chip[row] = both.astype(BF16).reshape(4, 16, width)
            return carry

        lax.fori_loop(0, count, body, 0)
        rows = pl.ds(lo, count)
        axis = COLOR_AXES[color][0]
        away, back = (1, 3) if half == 0 else (3, 1)
        relays[color, half] = push(chip.at[rows, 2], relay.at[rows], peer(axis, away))
        cleans[color, half] = push(chip.at[rows, back], line.at[half, rows], peer(axis, back))
        if half == 1:
            z_one[color] = line_z(color, 1, z_own[color] + z_swap[color])

    with jax.named_scope("dispatch0"):
        for chunk, load in zip(chunks[:1], loads[:1]):
            load.wait()
            dispatch(chunk)
    with jax.named_scope("barrier"):
        pl.semaphore_wait(barrier, len(neighbours))
    pending = start_swap(chunks[0])
    for index in range(len(chunks)):
        following = None
        if index + 1 < len(chunks):
            with jax.named_scope("dispatch"):
                loads[index + 1].wait()
                dispatch(chunks[index + 1])
            following = start_swap(chunks[index + 1])
        with jax.named_scope("chip"):
            start_line(chunks[index], pending)
        pending = following
    store_comb = pltpu.make_async_copy(comb, comb_hbm, local_sem.at[8])
    store_comb.start()

    seconds = {}
    for chunk in chunks:
        color, half, lo, count = chunk
        axis = COLOR_AXES[color][0]
        with jax.named_scope("relay"):
            relays[color, half].wait_recv()
            away = 1 if half == 0 else 3

            def body(step, carry):
                row = lo + step
                chip[row, away] = (chip[row, away].astype(F32) + relay[row].astype(F32)).astype(BF16)
                return carry

            lax.fori_loop(0, count, body, 0)
            rows = pl.ds(lo, count)
            seconds[color, half] = push(chip.at[rows, away], line.at[1 - half, rows], peer(axis, away))
    left = lax.broadcasted_iota(jnp.int32, (256, 256), 0)
    right = lax.broadcasted_iota(jnp.int32, (256, 256), 1)
    turn = jnp.where(((left >> 4) == (right & 15)) & ((left & 15) == (right >> 4)), 1.0, 0.0).astype(BF16)

    twos, z_two = {}, {}
    for color in range(3):
        with jax.named_scope("one"):
            rows, start = COLOR_ROWS[color], COLOR_START[color]
            span = pl.ds(start, rows)
            for half in range(2):
                cleans[color, half].wait_recv()
                seconds[color, half].wait_recv()
            z_two[color] = line_z(color, 2, sum_z(color, 1, z_one[color]))
            total = chip[span, 0].astype(F32) + line[0, span].astype(F32) + line[1, span].astype(F32)
            total = total.astype(BF16).reshape(rows * 16, width)
            turned = jnp.dot(turn[:, : rows * 16], total, preferred_element_type=F32)
            two_out[color] = turned.astype(BF16).reshape(4, 4, 16, width)
            axis = COLOR_AXES[color][1]
            twos[color] = [push(two_out.at[color, step], two_in.at[color, step - 1], peer(axis, step)) for step in (1, 2, 3)]
    threes, z_three = {}, {}
    for color in range(3):
        with jax.named_scope("two"):
            z_three[color] = line_z(color, 3, sum_z(color, 2, z_two[color]))
            total = two_out[color, 0].astype(F32)
            for step in (1, 2, 3):
                twos[color][step - 1].wait_recv()
                total = total + two_in[color, step - 1].astype(F32)
            three_out[color] = total.astype(BF16)
            axis = COLOR_AXES[color][2]
            threes[color] = [push(three_out.at[color, step], three_in.at[color, step - 1], peer(axis, step)) for step in (1, 2, 3)]
    slot_in = []
    for color in range(3):
        with jax.named_scope("three"):
            z_sum = sum_z(color, 3, z_three[color])
            total = three_out[color, 0].astype(F32)
            for step in (1, 2, 3):
                threes[color][step - 1].wait_recv()
                total = total + three_in[color, step - 1].astype(F32)
            slot_in.append((total / z_sum[:, :1]).astype(BF16))
    slot_in = jnp.concatenate(slot_in, axis=0)

    with jax.named_scope("expert"):
        load_in.wait()
        load_out.wait()
        slot_out = jnp.zeros((48, width), F32)
        for piece in range(3):
            cols = pl.ds(piece * 512, 512)
            hidden = jnp.dot(slot_in, win[:, cols], preferred_element_type=F32)
            hidden = jax.nn.gelu(hidden).astype(BF16)
            slot_out = slot_out + jnp.dot(hidden, wout[cols, :], preferred_element_type=F32)
        slot_out = slot_out.astype(BF16)
    firsts = {}
    for color in range(3):
        with jax.named_scope("first"):
            lanes[color, 0, 0] = slot_out[16 * color : 16 * color + 16]
            axis = COLOR_AXES[color][2]
            firsts[color] = [push(lanes.at[color, 0, 0], lanes.at[color, 0, 4 - step], peer(axis, step)) for step in (1, 2, 3)]
    nexts = {}
    for color in range(3):
        with jax.named_scope("next"):
            for copy in firsts[color]:
                copy.wait_recv()
            axis = COLOR_AXES[color][1]
            nexts[color] = [push(lanes.at[color, 0], lanes.at[color, 4 - step], peer(axis, step)) for step in (1, 2, 3)]
    outs, across = {}, {color: [] for color in range(3)}

    def halves(color):
        start, rows, cut = COLOR_START[color], COLOR_ROWS[color], COLOR_HALF[color]
        return pl.ds(start, cut), pl.ds(start + cut, rows - cut)

    for color in range(3):
        with jax.named_scope("turn"):
            rows, start = COLOR_ROWS[color], COLOR_START[color]
            for copy in nexts[color]:
                copy.wait_recv()
            turned = jnp.dot(turn[: rows * 16], lanes[color].reshape(256, width), preferred_element_type=F32)
            gat[pl.ds(start, rows), 0, 0] = turned.astype(BF16).reshape(rows, 16, width)
            early, late = halves(color)
            axis = COLOR_AXES[color][0]
            up, down = peer(axis, 1), peer(axis, 3)
            outs[color] = [
                push(gat.at[early, 0, 0], gat.at[early, 0, 3], up),
                push(gat.at[late, 0, 0], gat.at[late, 0, 1], down),
                push(gat.at[late, 0, 0], gat.at[late, 0, 3], up),
                push(gat.at[early, 0, 0], gat.at[early, 0, 1], down),
            ]
            span = pl.ds(start, rows)
            across[color].append(push(gat.at[span, 0, 0], gat.at[span, 1, 0], partner))
    hops = {}
    for color in range(3):
        early, late = halves(color)
        axis = COLOR_AXES[color][0]
        up, down = peer(axis, 1), peer(axis, 3)
        with jax.named_scope("hop"):
            outs[color][0].wait_recv()
            first = push(gat.at[early, 0, 3], gat.at[early, 0, 2], up)
            outs[color][1].wait_recv()
            second = push(gat.at[late, 0, 1], gat.at[late, 0, 2], down)
            hops[color] = [first, second]
            across[color].append(push(gat.at[early, 0, 3], gat.at[early, 1, 3], partner))
            across[color].append(push(gat.at[late, 0, 1], gat.at[late, 1, 1], partner))
    for color in range(3):
        early, late = halves(color)
        with jax.named_scope("late"):
            outs[color][2].wait_recv()
            across[color].append(push(gat.at[late, 0, 3], gat.at[late, 1, 3], partner))
            outs[color][3].wait_recv()
            across[color].append(push(gat.at[early, 0, 1], gat.at[early, 1, 1], partner))
    for color in range(3):
        early, late = halves(color)
        with jax.named_scope("last"):
            hops[color][0].wait_recv()
            across[color].append(push(gat.at[early, 0, 2], gat.at[early, 1, 2], partner))
            hops[color][1].wait_recv()
            across[color].append(push(gat.at[late, 0, 2], gat.at[late, 1, 2], partner))
    stores = [store_comb]
    for color in range(3):
        with jax.named_scope("store"):
            for copy in across[color]:
                copy.wait_recv()
            span = pl.ds(COLOR_START[color], COLOR_ROWS[color])
            store = pltpu.make_async_copy(gat.at[span], gat_hbm.at[span], local_sem.at[9 + color])
            store.start()
            stores.append(store)
    with jax.named_scope("drain"):
        for copy in copies:
            copy.wait_send()
        for store in stores:
            store.wait()
def combine_kernel(len_ref, comb_ref, gat_ref, y_ref):
    count, tok_count, _ = comb_ref.shape
    base = pl.program_id(0) * count
    position = lax.axis_index("seq") * tok_count + lax.broadcasted_iota(jnp.int32, (tok_count, 1), 0)
    for step in range(count):
        mixed = jnp.dot(comb_ref[step], gat_ref[step], preferred_element_type=F32).astype(BF16)
        y_ref[step] = jnp.where(position < len_ref[base + step], mixed, jnp.zeros_like(mixed))


def solution(mesh):
    def shard_body(tok_blk, len_blk, slot_params, logit_scale, w_in_blk, w_out_blk):
        rows, toks, width = tok_blk.shape
        ff = w_in_blk.shape[2]
        slots = slot_params.shape[1]
        smem = pl.BlockSpec(memory_space=pltpu.SMEM)
        vmem = pl.BlockSpec(memory_space=pltpu.VMEM)
        hbm = pl.BlockSpec(memory_space=pl.ANY)
        comb, gat = pl.pallas_call(
            slots_kernel,
            name="slots",
            out_shape=(
                jax.ShapeDtypeStruct((rows, toks, slots), BF16),
                jax.ShapeDtypeStruct((rows, 2, 4, 16, width), BF16),
            ),
            in_specs=[smem, smem, hbm, vmem, hbm, hbm],
            out_specs=(hbm, hbm),
            scratch_shapes=[
                pltpu.VMEM((rows, toks, width), BF16),
                pltpu.VMEM((width, ff), BF16),
                pltpu.VMEM((ff, width), BF16),
                pltpu.VMEM((rows, toks, slots), BF16),
                pltpu.VMEM((rows, 2, 64, width), BF16),
                pltpu.VMEM((rows, 64, width), BF16),
                pltpu.VMEM((rows, 4, 16, width), BF16),
                pltpu.VMEM((rows, 16, width), BF16),
                pltpu.VMEM((2, rows, 16, width), BF16),
                pltpu.VMEM((3, 4, 4, 16, width), BF16),
                pltpu.VMEM((3, 3, 4, 16, width), BF16),
                pltpu.VMEM((3, 4, 16, width), BF16),
                pltpu.VMEM((3, 3, 16, width), BF16),
                pltpu.VMEM((3, 16, slots), F32),
                pltpu.VMEM((4, 3, 16, slots), F32),
                pltpu.VMEM((3, 16, slots), F32),
                pltpu.VMEM((3, 3, 3, 16, slots), F32),
                pltpu.VMEM((3, 4, 4, 16, width), BF16),
                pltpu.VMEM((rows, 2, 4, 16, width), BF16),
                pltpu.SemaphoreType.DMA((COPIES,)),
                pltpu.SemaphoreType.DMA((COPIES,)),
                pltpu.SemaphoreType.DMA((12,)),
            ],
            compiler_params=pltpu.CompilerParams(collective_id=0, has_side_effects=True, vmem_limit_bytes=60 * 1024 * 1024),
        )(len_blk, logit_scale, tok_blk, slot_params, w_in_blk, w_out_blk)
        gat = gat.reshape(rows, slots, width)
        block = 4
        return pl.pallas_call(
            combine_kernel,
            name="combine",
            out_shape=jax.ShapeDtypeStruct((rows, toks, width), BF16),
            grid=(rows // block,),
            in_specs=[
                smem,
                pl.BlockSpec((block, toks, slots), lambda i: (i, 0, 0)),
                pl.BlockSpec((block, slots, width), lambda i: (i, 0, 0)),
            ],
            out_specs=pl.BlockSpec((block, toks, width), lambda i: (i, 0, 0)),
        )(len_blk, comb, gat)

    return jax.shard_map(
        shard_body,
        mesh=mesh,
        in_specs=(P("data", "seq", None), P("data"), P(None, None), P(None), P("seq", None, None), P("seq", None, None)),
        out_specs=P("data", "seq", None),
        check_vma=False,
    )
```

```python
import functools

import jax
import jax.numpy as jnp
from jax import lax
from jax.experimental import pallas as pl
from jax.experimental.pallas import tpu as pltpu
from jax.sharding import PartitionSpec as P

F32, BF16 = jnp.float32, jnp.bfloat16
COLOR_ROWS = (11, 11, 10)
COLOR_START = (0, 11, 22)
COLOR_HALF = (6, 6, 5)
STRIDE = {"z": 32, "y": 8, "x": 2}
COLOR_AXES = (("z", "y", "x"), ("y", "x", "z"), ("x", "z", "y"))
COPIES = 160


def slots_kernel(
    len_ref, scale_ref, tok_hbm, phi_ref, win_hbm, wout_hbm,
    comb, gat,
    tok, win, wout, part, swap, chip, relay, line,
    two_out, two_in, three_out, three_in, z_own, z_out, z_swap, z_in, lanes,
    send_sem, recv_sem, local_sem,
):
    num_rows, tok_count, width = tok.shape
    me = lax.axis_index("seq")
    core = lax.rem(me, 2)
    at = {axis: lax.rem(lax.div(me, stride), 4) for axis, stride in STRIDE.items()}
    partner = me + 1 - 2 * core

    def peer(axis, step):
        return me + (lax.rem(at[axis] + step, 4) - at[axis]) * STRIDE[axis]

    copies = []

    def push(src, dst, device):
        index = len(copies)
        copy = pltpu.make_async_remote_copy(
            src_ref=src, dst_ref=dst, send_sem=send_sem.at[index], recv_sem=recv_sem.at[index],
            device_id={"seq": device}, device_id_type=pl.DeviceIdType.MESH,
        )
        copy.start()
        copies.append(copy)
        return copy

    chunks = []
    for half in range(2):
        for color in range(3):
            start, rows, cut = COLOR_START[color], COLOR_ROWS[color], COLOR_HALF[color]
            chunks.append((color, half, start + half * cut, cut if half == 0 else rows - cut))

    barrier = pltpu.get_barrier_semaphore()
    neighbours = [partner] + [peer(axis, step) for axis in STRIDE for step in (1, 2, 3)]
    for other in neighbours:
        pl.semaphore_signal(barrier, inc=1, device_id={"seq": other}, device_id_type=pl.DeviceIdType.MESH)

    loads = []
    for index, (_, _, lo, count) in enumerate(chunks):
        load = pltpu.make_async_copy(tok_hbm.at[pl.ds(lo, count)], tok.at[pl.ds(lo, count)], local_sem.at[index])
        load.start()
        loads.append(load)
    load_in = pltpu.make_async_copy(win_hbm.at[0], win, local_sem.at[6])
    load_out = pltpu.make_async_copy(wout_hbm.at[0], wout, local_sem.at[7])
    load_in.start()
    load_out.start()

    with jax.named_scope("setup"):
        params = phi_ref[...].astype(F32)
        col_inv = lax.rsqrt(jnp.sum(params * params, axis=0, keepdims=True) + 1e-6)
        phi = (params * (scale_ref[0] * col_inv)).astype(BF16)
        slot = lax.broadcasted_iota(jnp.int32, (128, 128), 0)
        place = lax.broadcasted_iota(jnp.int32, (128, 128), 1)
        phis = []
        for color in range(3):
            owner = (core + (place >> 6)) & 1
            for depth, axis in enumerate(COLOR_AXES[color]):
                owner = owner + STRIDE[axis] * ((at[axis] + (place >> (4 - 2 * depth))) & 3)
            pick = jnp.where(slot == owner, 1.0, 0.0).astype(BF16)
            phis.append(jnp.dot(phi, pick, preferred_element_type=F32).astype(BF16))
        z_own[...] = jnp.ones_like(z_own)
        position = me * tok_count + lax.broadcasted_iota(jnp.int32, (tok_count, 128), 0)
    def dispatch(chunk):
        color, _, lo, count = chunk
        xs = [tok[lo + step] for step in range(count)]
        squares = [jnp.sum(x.astype(F32) * x.astype(F32), axis=-1, keepdims=True) for x in xs]
        norms = [(x.astype(F32) * lax.rsqrt(square + 1e-6)).astype(BF16) for x, square in zip(xs, squares)]
        weights = [jnp.exp(jnp.dot(norm, phis[color], preferred_element_type=F32)) for norm in norms]
        masked = [jnp.where(position < len_ref[lo + step], weight, 0.0) for step, weight in enumerate(weights)]
        totals = [
            lax.dot_general(weight.astype(BF16), x, (((0,), (0,)), ((), ())), preferred_element_type=F32).astype(BF16)
            for weight, x in zip(masked, xs)
        ]
        for step in range(count):
            row = lo + step
            part[row, 0] = totals[step][:64]
            part[row, 1] = totals[step][64:]
            at_row = row - COLOR_START[color]
            z_own[color, at_row : at_row + 1, :] = jnp.sum(masked[step], axis=0, keepdims=True)
            comb[row] = (weights[step] / jnp.sum(weights[step], axis=-1, keepdims=True)).astype(BF16)

    def start_swap(chunk):
        color, half, lo, count = chunk
        rows = pl.ds(lo, count)
        out = [push(part.at[rows, 1], swap.at[rows], partner)]
        if half == 1:
            z_out[0, color] = pltpu.roll(z_own[color], 64, 1)
            out.append(push(z_out.at[0, color], z_swap.at[color], partner))
        return out

    def line_z(color, phase, total):
        z_out[phase, color] = total
        axis = COLOR_AXES[color][phase - 1]
        return [push(z_out.at[phase, color], z_in.at[phase - 1, color, step - 1], peer(axis, step)) for step in (1, 2, 3)]

    def sum_z(color, phase, arrivals):
        total = z_out[phase, color]
        for step in (1, 2, 3):
            arrivals[step - 1].wait_recv()
            shift = 128 - step * (64 >> (2 * phase))
            total = total + pltpu.roll(z_in[phase - 1, color, step - 1], shift, 1)
        return total

    relays, cleans, z_one = {}, {}, {}

    def start_line(chunk, arrivals):
        color, half, lo, count = chunk
        for copy in arrivals:
            copy.wait_recv()

        def body(step, carry):
            row = lo + step
            both = part[row, 0].astype(F32) + swap[row].astype(F32)
            chip[row] = both.astype(BF16).reshape(4, 16, width)
            return carry

        lax.fori_loop(0, count, body, 0)
        rows = pl.ds(lo, count)
        axis = COLOR_AXES[color][0]
        away, back = (1, 3) if half == 0 else (3, 1)
        relays[color, half] = push(chip.at[rows, 2], relay.at[rows], peer(axis, away))
        cleans[color, half] = push(chip.at[rows, back], line.at[half, rows], peer(axis, back))
        if half == 1:
            z_one[color] = line_z(color, 1, z_own[color] + z_swap[color])

    with jax.named_scope("dispatch0"):
        for chunk, load in zip(chunks[:1], loads[:1]):
            load.wait()
            dispatch(chunk)
    with jax.named_scope("barrier"):
        pl.semaphore_wait(barrier, len(neighbours))
    pending = start_swap(chunks[0])
    for index in range(len(chunks)):
        following = None
        if index + 1 < len(chunks):
            with jax.named_scope("dispatch"):
                loads[index + 1].wait()
                dispatch(chunks[index + 1])
            following = start_swap(chunks[index + 1])
        with jax.named_scope("chip"):
            start_line(chunks[index], pending)
        pending = following

    seconds = {}
    for chunk in chunks:
        color, half, lo, count = chunk
        axis = COLOR_AXES[color][0]
        with jax.named_scope("relay"):
            relays[color, half].wait_recv()
            away = 1 if half == 0 else 3

            def body(step, carry):
                row = lo + step
                chip[row, away] = (chip[row, away].astype(F32) + relay[row].astype(F32)).astype(BF16)
                return carry

            lax.fori_loop(0, count, body, 0)
            rows = pl.ds(lo, count)
            seconds[color, half] = push(chip.at[rows, away], line.at[1 - half, rows], peer(axis, away))
    left = lax.broadcasted_iota(jnp.int32, (256, 256), 0)
    right = lax.broadcasted_iota(jnp.int32, (256, 256), 1)
    turn = jnp.where(((left >> 4) == (right & 15)) & ((left & 15) == (right >> 4)), 1.0, 0.0).astype(BF16)

    twos, z_two = {}, {}
    for color in range(3):
        with jax.named_scope("one"):
            rows, start = COLOR_ROWS[color], COLOR_START[color]
            span = pl.ds(start, rows)
            for half in range(2):
                cleans[color, half].wait_recv()
                seconds[color, half].wait_recv()
            z_two[color] = line_z(color, 2, sum_z(color, 1, z_one[color]))
            total = chip[span, 0].astype(F32) + line[0, span].astype(F32) + line[1, span].astype(F32)
            total = total.astype(BF16).reshape(rows * 16, width)
            turned = jnp.dot(turn[:, : rows * 16], total, preferred_element_type=F32)
            two_out[color] = turned.astype(BF16).reshape(4, 4, 16, width)
            axis = COLOR_AXES[color][1]
            twos[color] = [push(two_out.at[color, step], two_in.at[color, step - 1], peer(axis, step)) for step in (1, 2, 3)]
    threes, z_three = {}, {}
    for color in range(3):
        with jax.named_scope("two"):
            z_three[color] = line_z(color, 3, sum_z(color, 2, z_two[color]))
            total = two_out[color, 0].astype(F32)
            for step in (1, 2, 3):
                twos[color][step - 1].wait_recv()
                total = total + two_in[color, step - 1].astype(F32)
            three_out[color] = total.astype(BF16)
            axis = COLOR_AXES[color][2]
            threes[color] = [push(three_out.at[color, step], three_in.at[color, step - 1], peer(axis, step)) for step in (1, 2, 3)]
    slot_in = []
    for color in range(3):
        with jax.named_scope("three"):
            z_sum = sum_z(color, 3, z_three[color])
            total = three_out[color, 0].astype(F32)
            for step in (1, 2, 3):
                threes[color][step - 1].wait_recv()
                total = total + three_in[color, step - 1].astype(F32)
            slot_in.append((total / z_sum[:, :1]).astype(BF16))
    slot_in = jnp.concatenate(slot_in, axis=0)

    with jax.named_scope("expert"):
        load_in.wait()
        load_out.wait()
        slot_out = jnp.zeros((48, width), F32)
        for piece in range(3):
            cols = pl.ds(piece * 512, 512)
            hidden = jnp.dot(slot_in, win[:, cols], preferred_element_type=F32)
            hidden = jax.nn.gelu(hidden).astype(BF16)
            slot_out = slot_out + jnp.dot(hidden, wout[cols, :], preferred_element_type=F32)
        slot_out = slot_out.astype(BF16)
    firsts = {}
    for color in range(3):
        with jax.named_scope("first"):
            lanes[color, 0, 0] = slot_out[16 * color : 16 * color + 16]
            axis = COLOR_AXES[color][2]
            firsts[color] = [push(lanes.at[color, 0, 0], lanes.at[color, 0, 4 - step], peer(axis, step)) for step in (1, 2, 3)]
    nexts = {}
    for color in range(3):
        with jax.named_scope("next"):
            for copy in firsts[color]:
                copy.wait_recv()
            axis = COLOR_AXES[color][1]
            nexts[color] = [push(lanes.at[color, 0], lanes.at[color, 4 - step], peer(axis, step)) for step in (1, 2, 3)]
    outs, across = {}, {color: [] for color in range(3)}

    def halves(color):
        start, rows, cut = COLOR_START[color], COLOR_ROWS[color], COLOR_HALF[color]
        return pl.ds(start, cut), pl.ds(start + cut, rows - cut)

    for color in range(3):
        with jax.named_scope("turn"):
            rows, start = COLOR_ROWS[color], COLOR_START[color]
            for copy in nexts[color]:
                copy.wait_recv()
            turned = jnp.dot(turn[: rows * 16], lanes[color].reshape(256, width), preferred_element_type=F32)
            gat[pl.ds(start, rows), 0, 0] = turned.astype(BF16).reshape(rows, 16, width)
            early, late = halves(color)
            axis = COLOR_AXES[color][0]
            up, down = peer(axis, 1), peer(axis, 3)
            outs[color] = [
                push(gat.at[early, 0, 0], gat.at[early, 0, 3], up),
                push(gat.at[late, 0, 0], gat.at[late, 0, 1], down),
                push(gat.at[late, 0, 0], gat.at[late, 0, 3], up),
                push(gat.at[early, 0, 0], gat.at[early, 0, 1], down),
            ]
            span = pl.ds(start, rows)
            across[color].append(push(gat.at[span, 0, 0], gat.at[span, 1, 0], partner))
    hops = {}
    for color in range(3):
        early, late = halves(color)
        axis = COLOR_AXES[color][0]
        up, down = peer(axis, 1), peer(axis, 3)
        with jax.named_scope("hop"):
            outs[color][0].wait_recv()
            first = push(gat.at[early, 0, 3], gat.at[early, 0, 2], up)
            outs[color][1].wait_recv()
            second = push(gat.at[late, 0, 1], gat.at[late, 0, 2], down)
            hops[color] = [first, second]
            across[color].append(push(gat.at[early, 0, 3], gat.at[early, 1, 3], partner))
            across[color].append(push(gat.at[late, 0, 1], gat.at[late, 1, 1], partner))
    for color in range(3):
        early, late = halves(color)
        with jax.named_scope("late"):
            outs[color][2].wait_recv()
            across[color].append(push(gat.at[late, 0, 3], gat.at[late, 1, 3], partner))
            outs[color][3].wait_recv()
            across[color].append(push(gat.at[early, 0, 1], gat.at[early, 1, 1], partner))
    for color in range(3):
        early, late = halves(color)
        with jax.named_scope("last"):
            hops[color][0].wait_recv()
            across[color].append(push(gat.at[early, 0, 2], gat.at[early, 1, 2], partner))
            hops[color][1].wait_recv()
            across[color].append(push(gat.at[late, 0, 2], gat.at[late, 1, 2], partner))
    with jax.named_scope("across"):
        for color in range(3):
            for copy in across[color]:
                copy.wait_recv()
    with jax.named_scope("drain"):
        for copy in copies:
            copy.wait_send()


def combine_kernel(len_ref, comb, gat, y_hbm, y, sem):
    num_rows, tok_count, width = y.shape
    position = lax.axis_index("seq") * tok_count + lax.broadcasted_iota(jnp.int32, (tok_count, 1), 0)
    group = 4
    stores = []
    for first in range(0, num_rows, group):
        for row in range(first, first + group):
            mixed = jnp.dot(comb[row], gat[row].reshape(128, width), preferred_element_type=F32).astype(BF16)
            y[row] = jnp.where(position < len_ref[row], mixed, jnp.zeros_like(mixed))
        span = pl.ds(first, group)
        store = pltpu.make_async_copy(y.at[span], y_hbm.at[span], sem.at[first // group])
        store.start()
        stores.append(store)
    for store in stores:
        store.wait()


def solution(mesh):
    def shard_body(tok_blk, len_blk, slot_params, logit_scale, w_in_blk, w_out_blk):
        rows, toks, width = tok_blk.shape
        ff = w_in_blk.shape[2]
        slots = slot_params.shape[1]
        smem = pl.BlockSpec(memory_space=pltpu.SMEM)
        vmem = pl.BlockSpec(memory_space=pltpu.VMEM)
        hbm = pl.BlockSpec(memory_space=pltpu.HBM)
        comb, gat = pl.pallas_call(
            slots_kernel,
            name="slots",
            out_shape=(
                pltpu.VMEM((rows, toks, slots), BF16),
                pltpu.VMEM((rows, 2, 4, 16, width), BF16),
            ),
            in_specs=[smem, smem, hbm, vmem, hbm, hbm],
            out_specs=(vmem, vmem),
            scratch_shapes=[
                pltpu.VMEM((rows, toks, width), BF16),
                pltpu.VMEM((width, ff), BF16),
                pltpu.VMEM((ff, width), BF16),
                pltpu.VMEM((rows, 2, 64, width), BF16),
                pltpu.VMEM((rows, 64, width), BF16),
                pltpu.VMEM((rows, 4, 16, width), BF16),
                pltpu.VMEM((rows, 16, width), BF16),
                pltpu.VMEM((2, rows, 16, width), BF16),
                pltpu.VMEM((3, 4, 4, 16, width), BF16),
                pltpu.VMEM((3, 3, 4, 16, width), BF16),
                pltpu.VMEM((3, 4, 16, width), BF16),
                pltpu.VMEM((3, 3, 16, width), BF16),
                pltpu.VMEM((3, 16, slots), F32),
                pltpu.VMEM((4, 3, 16, slots), F32),
                pltpu.VMEM((3, 16, slots), F32),
                pltpu.VMEM((3, 3, 3, 16, slots), F32),
                pltpu.VMEM((3, 4, 4, 16, width), BF16),
                pltpu.SemaphoreType.DMA((COPIES,)),
                pltpu.SemaphoreType.DMA((COPIES,)),
                pltpu.SemaphoreType.DMA((8,)),
            ],
            compiler_params=pltpu.CompilerParams(collective_id=0, has_side_effects=True, vmem_limit_bytes=56 * 1024 * 1024),
        )(len_blk, logit_scale, tok_blk, slot_params, w_in_blk, w_out_blk)
        return pl.pallas_call(
            combine_kernel,
            name="combine",
            out_shape=jax.ShapeDtypeStruct((rows, toks, width), BF16),
            in_specs=[smem, vmem, vmem],
            out_specs=hbm,
            scratch_shapes=[pltpu.VMEM((rows, toks, width), BF16), pltpu.SemaphoreType.DMA((8,))],
            compiler_params=pltpu.CompilerParams(vmem_limit_bytes=16 * 1024 * 1024),
        )(len_blk, comb, gat)

    return jax.shard_map(
        shard_body,
        mesh=mesh,
        in_specs=(P("data", "seq", None), P("data"), P(None, None), P(None), P("seq", None, None), P("seq", None, None)),
        out_specs=P("data", "seq", None),
        check_vma=False,
    )
```
